32 devices in a mesh: dp: 2 (over x), fsdp: 16 (over z, y, core).
Axes of the slice: x: 2, y: 2, z: 4, core: 2. Of those that a mesh axis runs over, the one named last changes fastest.
Arguments:
- hidden_states: bfloat16 [32, 1024, 768], P(('dp', 'fsdp')), may hold values from -6 to 6
- condition: bfloat16 [32, 128], P(('dp', 'fsdp')), may hold values from -6 to 6
- absorbed: int32 [32, 1024], P(('dp', 'fsdp')), may hold values 0 or 1
- positions: int32 [32, 1024], P(('dp', 'fsdp')), may hold values from 0 to 2047, as said below
- modulator: bfloat16 [128, 4608], P('fsdp'), may hold values from -0.5 to 0.5
- offsets: bfloat16 [4608], P('fsdp'), may hold values from -3 to 3
- prescale: bfloat16 [768], P('fsdp'), may hold values from 0.5 to 1.5
- projector: bfloat16 [768, 2304], P('fsdp'), may hold values from -0.3125 to 0.3125
- merger: bfloat16 [768, 768], P('fsdp'), may hold values from -0.625 to 0.625
- midscale: bfloat16 [768], P('fsdp'), may hold values from 0.5 to 1.5
- expander: bfloat16 [768, 3072], P('fsdp'), may hold values from -0.21875 to 0.21875
- thresholds: bfloat16 [3072], P('fsdp'), may hold values from -3 to 3
- contractor: bfloat16 [3072, 768], P('fsdp'), may hold values from -0.109375 to 0.109375
- baseline: bfloat16 [768], P('fsdp'), may hold values from -3 to 3
- absorber: bfloat16 [768], P('fsdp'), may hold values from -6 to 6
- cotangent: bfloat16 [32, 1024, 768], P(('dp', 'fsdp')), may hold values from -6 to 6
Outputs:
- block_output: bfloat16 [32, 1024, 768], P(('dp', 'fsdp'))
- grad_hidden: float32 [32, 1024, 768], P(('dp', 'fsdp'))
- grad_condition: float32 [32, 128], P(('dp', 'fsdp'))
- grad_modulator: float32 [128, 4608], P('fsdp')
- grad_offsets: float32 [4608], P('fsdp')
- grad_prescale: float32 [768], P('fsdp')
- grad_projector: float32 [768, 2304], P('fsdp')
- grad_merger: float32 [768, 768], P('fsdp')
- grad_midscale: float32 [768], P('fsdp')
- grad_expander: float32 [768, 3072], P('fsdp')
- grad_thresholds: float32 [3072], P('fsdp')
- grad_contractor: float32 [3072, 768], P('fsdp')
- grad_baseline: float32 [768], P('fsdp')
- grad_absorber: float32 [768], P('fsdp')
The draws below stay inside these ranges and needn't reach their ends.
Inputs may be any that keep to these rules, and one draw needn't show every extreme that they name: `absorbed`: 1 marks a token in the absorbing state, 0 any other. Along each sequence the positions rise by 1 or 2 from one token to the next; the first is 0 or 1. The first sequence starts at 0, and the last sequence rises by 2 at every token.
All inputs are finite; a program needn't handle non-finite values. No bound on the sum of `absorbed` on one device may be relied on, other than what follows from the above.
Results may differ from the reference program's by a relative error of at most 0.039.
Values may be sent and summed in bfloat16 or wider, within the bound.
A program may use at most 192 MiB of HBM per device.

```python
import jax
import jax.numpy as jnp
from jax import lax

D = 768
HEADS = 12
HD = 64
FF = 3072
C = 128
L = 1024
SEQS = 32


def draw_positions(key, part):
    increments = jax.random.randint(key, (SEQS, L), 1, 3)
    increments = increments.at[0, 0].set(1)
    increments = increments.at[SEQS - 1].set(2)
    return (jnp.cumsum(increments, axis=1) - 1).astype(jnp.int32)


def touch_ends(array, own_key, low, largest):
    place = [jax.random.randint(jax.random.fold_in(own_key, axis), (), 0, length) for axis, length in enumerate(array.shape)]
    widest = array.shape.index(max(array.shape))
    neighbour = place[:widest] + [(place[widest] + 1) % array.shape[widest]] + place[widest + 1:]
    return array.at[tuple(place)].set(low).at[tuple(neighbour)].set(largest)


def with_spikes(entries, own_key, source, target, parts, factor):
    owner, partner = [(jnp.arange(entries.shape[dim]) // (entries.shape[dim] // parts)).reshape([-1 if axis == dim else 1 for axis in range(entries.ndim)]) for dim in (source, target)]
    chosen = jax.random.permutation(own_key, parts)[partner]
    strong = (owner == chosen) | (owner == (partner + parts // 2) % parts)
    return jnp.where(strong, factor * entries, entries)


def block_levels(key, dims, cuts, low, top_value):
    def one(dim, shards_of):
        heights = jax.random.uniform(jax.random.fold_in(jax.random.fold_in(key, 6), dim), (shards_of,), jnp.float32, low / len(cuts), top_value / len(cuts))
        return jnp.repeat(jnp.exp(heights), dims[dim] // shards_of).reshape((-1,) + (1,) * (len(dims) - dim - 1))

    level = one(*cuts[0])
    for cut in cuts[1:]:
        level = level * one(*cut)
    return level


def noise(key, extent, deviation, limit, pieces=(), kind=jnp.bfloat16):
    result = deviation * jax.random.normal(key, extent, jnp.float32)
    if pieces:
        result = result * block_levels(key, extent, pieces, -0.22, 0.18)
    return jnp.clip(result, -limit, limit).astype(kind)


def noise_with(own_key, extent, width, limit, pieces, heavy, kind=jnp.bfloat16):
    values = width * jax.random.normal(own_key, extent, jnp.float32)
    if pieces:
        values = values * block_levels(own_key, extent, pieces, -0.22, 0.18)
    return jnp.clip(with_spikes(values, jax.random.fold_in(own_key, 3), *heavy), -limit, limit).astype(kind)


def setup_inputs(seed: int = 0) -> dict:
    arg_keys = jax.random.split(jax.random.key(seed), 17)
    hidden_states = noise(arg_keys[0], (SEQS, L, D), 1.0, 6.0, ((0, 32),))
    condition = noise(arg_keys[1], (SEQS, C), 1.0, 6.0, ((0, 32),))
    absorbed = touch_ends((jax.random.randint(arg_keys[2], (SEQS, L), 0, 2) < 1).astype(jnp.int32), jax.random.fold_in(arg_keys[2], 1), 0, 1)
    positions = draw_positions(jax.random.fold_in(arg_keys[16], 71), 0)
    modulator = noise(arg_keys[4], (C, 6 * D), C ** -0.5, 0.5, ((0, 16),))
    offsets = noise(arg_keys[5], (6 * D,), 0.5, 3.0, ((0, 16),))
    prescale = jnp.clip(1.0 + 0.1 * jax.random.normal(arg_keys[6], (D,), jnp.float32), 0.5, 1.5).astype(jnp.bfloat16)
    projector = noise(arg_keys[7], (D, 3 * D), (D // 2) ** -0.5, 0.3125, ((0, 16),))
    merger = noise(arg_keys[8], (D, D), (D // 8) ** -0.5, 0.625, ((0, 16),))
    midscale = jnp.clip(1.0 + 0.1 * jax.random.normal(arg_keys[9], (D,), jnp.float32), 0.5, 1.5).astype(jnp.bfloat16)
    expander = noise(arg_keys[10], (D, FF), D ** -0.5, 0.21875, ((0, 16),))
    thresholds = noise(arg_keys[11], (FF,), 0.5, 3.0, ((0, 16),))
    contractor = noise(arg_keys[12], (FF, D), FF ** -0.5, 0.109375, ((0, 16),))
    baseline = noise(arg_keys[13], (D,), 0.5, 3.0, ((0, 16),))
    absorber = noise(arg_keys[14], (D,), 1.0, 6.0, ((0, 16),))
    cotangent = noise_with(arg_keys[15], (SEQS, L, D), 1.0, 6.0, ((0, 32),), (0, 2, 32, 2.75))
    return {"hidden_states": hidden_states, "condition": condition, "absorbed": absorbed, "positions": positions, "modulator": modulator, "offsets": offsets, "prescale": prescale, "projector": projector, "merger": merger, "midscale": midscale, "expander": expander, "thresholds": thresholds, "contractor": contractor, "baseline": baseline, "absorber": absorber, "cotangent": cotangent}


@jax.custom_vjp
def low(v):
    return lax.optimization_barrier(v.astype(jnp.bfloat16)).astype(jnp.float32)

@jax.custom_vjp
def low_back(v):
    return v

def low_keep(v):
    return (low(v), None)

def low_pass(kept, grad):
    return (grad,)

def back_keep(v):
    return (v, None)

def back_low(kept, grad):
    return (low(grad),)
low.defvjp(low_keep, low_pass)
low_back.defvjp(back_keep, back_low)

def precise(left, right):
    return jnp.dot(left, right, precision=lax.Precision.HIGHEST, preferred_element_type=jnp.float32)

def norm_shift(values, gain, shift, scale):
    mean = lax.optimization_barrier(jnp.mean(values, -1, keepdims=True))
    centered = values - mean
    variance = lax.optimization_barrier(jnp.mean(centered * centered, -1, keepdims=True))
    return centered * lax.rsqrt(variance + 1e-05) * gain * (1.0 + scale) + shift

def rotate(values, cosine, sine):
    half = values.shape[-1] // 2
    first = values[..., :half]
    second = values[..., half:]
    return jnp.concatenate([first * cosine - second * sine, second * cosine + first * sine], -1)

def attend_head(operands):
    queries, keys, values = operands
    scores = low_back(precise(queries, keys.T) * HD ** (-0.5))
    probs = jax.nn.softmax(scores, axis=-1)
    return precise(low(probs), values)

def block(params, block_in, cond, cosine, sine):
    modulator, offsets, prescale, projector, merger, midscale, expander, thresholds, contractor, baseline = params
    groups = block_in.shape[0]
    modulation = precise(low(jax.nn.silu(cond)), modulator) + offsets
    shift_one, scale_one, gate_one, shift_two, scale_two, gate_two = jnp.split(modulation[:, None, :], 6, axis=-1)
    normed_one = low(norm_shift(block_in, prescale, shift_one, scale_one))
    united = low_back(precise(normed_one.reshape(-1, D), projector))
    heads_view = united.reshape(groups, L, 3, HEADS, HD)
    queries = low(rotate(heads_view[:, :, 0], cosine, sine))
    keys = low(rotate(heads_view[:, :, 1], cosine, sine))
    values = low(heads_view[:, :, 2])

    def per_head(tensor):
        return tensor.transpose(0, 2, 1, 3).reshape(groups * HEADS, L, HD)
    mixed = lax.map(jax.checkpoint(attend_head), (per_head(queries), per_head(keys), per_head(values)))
    attended = low_back(low(mixed.reshape(groups, HEADS, L, HD).transpose(0, 2, 1, 3).reshape(-1, D)))
    branch_one = low_back(precise(attended, merger)).reshape(groups, L, D)
    middle = block_in + gate_one * branch_one
    normed_two = low(norm_shift(middle, midscale, shift_two, scale_two)).reshape(-1, D)
    expanded = low_back(precise(normed_two, expander) + thresholds)
    activated = low(jax.nn.gelu(expanded, approximate=True))
    branch_two = low_back(precise(activated, contractor) + baseline).reshape(groups, L, D)
    return middle + gate_two * branch_two

def reference(hidden_states, condition, absorbed, positions, modulator, offsets, prescale, projector, merger, midscale, expander, thresholds, contractor, baseline, absorber, cotangent):
    params = tuple((weight.astype(jnp.float32) for weight in (modulator, offsets, prescale, projector, merger, midscale, expander, thresholds, contractor, baseline)))
    half = HD // 2
    inverse = 10000.0 ** (-jnp.arange(half, dtype=jnp.float32) / half)
    angles = positions.astype(jnp.float32)[..., None] * inverse
    cosine = jnp.cos(angles)[:, :, None, :]
    sine = jnp.sin(angles)[:, :, None, :]
    mask_rows = (absorbed == 1)[..., None]
    per_group = 4

    def regroup(tensor):
        return tensor.reshape((SEQS // per_group, per_group) + tensor.shape[1:])

    def forward(weights, absorber_row, hidden, cond):
        block_in = jnp.where(mask_rows, absorber_row, hidden)

        def run(operands):
            return block(weights, operands[0], operands[1], operands[2], operands[3])
        outputs = lax.map(jax.checkpoint(run), (regroup(block_in), regroup(cond), regroup(cosine), regroup(sine)))
        return outputs.reshape(SEQS, L, D)
    primal, pullback = jax.vjp(forward, params, absorber.astype(jnp.float32), hidden_states.astype(jnp.float32), condition.astype(jnp.float32))
    grad_params, grad_absorber, grad_hidden, grad_condition = pullback(cotangent.astype(jnp.float32))
    return (primal.astype(jnp.bfloat16), grad_hidden, grad_condition, grad_params[0], grad_params[1], grad_params[2], grad_params[3], grad_params[4], grad_params[5], grad_params[6], grad_params[7], grad_params[8], grad_params[9], grad_absorber)
```

```python
import functools
import math

import jax
import jax.numpy as jnp
from jax import lax
from jax.experimental import pallas as pl
from jax.experimental.pallas import tpu as pltpu
from jax.sharding import PartitionSpec as P

D = 768
HD = 64
PAIR = 2 * HD
BF = jnp.bfloat16
F32 = jnp.float32
LOG2E = math.log2(math.e)
LN2 = math.log(2.0)
NT = (((1,), (1,)), ((), ()))
VMEM_LIMIT = 60 << 20


def dot(a, b):
    return jnp.dot(a, b, preferred_element_type=F32)


def dot_nt(a, b):
    return lax.dot_general(a, b, NT, preferred_element_type=F32)


def dot_tn(a, b):
    return lax.dot_general(a, b, (((0,), (0,)), ((), ())), preferred_element_type=F32)


def gather_kernel(count, *refs):
    ins, outs = refs[:count], refs[count : 2 * count]
    own_sem, z_recv, z_up, z_down, y_recv, y_send, x_recv, x_send, c_recv, c_send = refs[2 * count :]
    x = lax.axis_index("dp")
    me = lax.axis_index("fsdp")
    z, y, core = me // 4, (me // 2) % 2, me % 2
    above, below, beside, partner = me + 4, me - 4, me + 2 - 4 * y, me + 1 - 2 * core
    barrier = pltpu.get_barrier_semaphore()

    def greet(dp, fsdp):
        pl.semaphore_signal(
            barrier, inc=1, device_id=(dp, fsdp), device_id_type=pl.DeviceIdType.MESH
        )

    greet(1 - x, me)
    greet(x, beside)
    greet(x, partner)
    pl.when(z < 3)(lambda: greet(x, above))
    pl.when(z > 0)(lambda: greet(x, below))
    pl.semaphore_wait(barrier, 3 + jnp.where(z < 3, 1, 0) + jnp.where(z > 0, 1, 0))

    def part(tensor, owner, first, parts):
        rows = ins[tensor].shape[0]
        third = rows // 3
        start = pl.multiple_of(owner * rows + first * third, 16)
        return outs[tensor].at[pl.ds(start, parts * third), :]

    def own(tensor, first, parts):
        third = ins[tensor].shape[0] // 3
        return ins[tensor].at[pl.ds(pl.multiple_of(first * third, 16), parts * third), :]

    def copy(source, target, send, recv, dp, fsdp):
        return pltpu.make_async_remote_copy(
            src_ref=source,
            dst_ref=target,
            send_sem=send,
            recv_sem=recv,
            device_id=(dp, fsdp),
            device_id_type=pl.DeviceIdType.MESH,
        )

    def place(step, flip):
        plane = z + step
        return plane, plane * 4 + (y + flip - 2 * y * flip) * 2 + core

    def z_copy(tensor, step, up):
        plane, owner = place(step, 0)
        source = own(tensor, x, 2) if step == 0 else part(tensor, owner, x, 2)
        send = (z_up if up else z_down).at[tensor, plane]
        return copy(
            source, part(tensor, owner, x, 2), send, z_recv.at[tensor, plane], x,
            above if up else below,
        )

    def y_copy(tensor, step):
        plane, owner = place(step, 0)
        source = own(tensor, x, 2) if step == 0 else part(tensor, owner, x, 2)
        return copy(
            source, part(tensor, owner, x, 2), y_send.at[tensor, plane],
            y_recv.at[tensor, plane], x, beside,
        )

    def x_copy(tensor, step, flip):
        plane, owner = place(step, flip)
        mine = step == 0 and flip == 0
        source = own(tensor, 2 * x, 1) if mine else part(tensor, owner, 2 * x, 1)
        return copy(
            source, part(tensor, owner, 2 * x, 1), x_send.at[tensor, flip, plane],
            x_recv.at[tensor, flip, plane], 1 - x, me,
        )

    def c_copy(tensor, step, flip, crossed):
        plane, owner = place(step, flip)
        first, parts = (2 - 2 * x, 1) if crossed else (x, 2)
        mine = step == 0 and flip == 0
        source = own(tensor, first, parts) if mine else part(tensor, owner, first, parts)
        kind = 1 if crossed else 0
        return copy(
            source, part(tensor, owner, first, parts), c_send.at[tensor, kind, flip, plane],
            c_recv.at[tensor, kind, flip, plane], x, partner,
        )

    def valid(step):
        return (z + step >= 0) & (z + step <= 3)

    steps = (0, -1, 1, -2, 2, -3, 3)

    def begin(tensor):
        pltpu.make_async_copy(
            ins[tensor], part(tensor, me, 0, 3), own_sem.at[tensor]
        ).start()
        pl.when(z < 3)(lambda: z_copy(tensor, 0, True).start())
        pl.when(z > 0)(lambda: z_copy(tensor, 0, False).start())
        y_copy(tensor, 0).start()
        c_copy(tensor, 0, 0, False).start()
        c_copy(tensor, 0, 0, True).start()

    def along_z(tensor):
        for step in steps[1:]:

            def arrive(step=step):
                z_copy(tensor, step, step < 0).wait_recv()
                if step < 0:
                    pl.when(z < 3)(lambda: z_copy(tensor, step, True).start())
                else:
                    pl.when(z > 0)(lambda: z_copy(tensor, step, False).start())
                y_copy(tensor, step).start()
                x_copy(tensor, step, 0).start()
                c_copy(tensor, step, 0, False).start()

            pl.when(valid(step))(arrive)

    def across_y(tensor):
        for step in steps:

            def arrive(step=step):
                y_arrived(tensor, step).wait_recv()
                x_copy(tensor, step, 1).start()
                c_copy(tensor, step, 1, False).start()

            pl.when(valid(step))(arrive)

    def y_arrived(tensor, step):
        plane, owner = place(step, 1)
        return copy(
            part(tensor, owner, x, 2), part(tensor, owner, x, 2), y_send.at[tensor, plane],
            y_recv.at[tensor, plane], x, beside,
        )

    def x_arrived(tensor, step, flip):
        plane, owner = place(step, flip)
        return copy(
            part(tensor, owner, 2 - 2 * x, 1), part(tensor, owner, 2 - 2 * x, 1),
            x_send.at[tensor, flip, plane], x_recv.at[tensor, flip, plane], 1 - x, me,
        )

    def across_x(tensor):
        for flip in (0, 1):
            for step in steps[1:] if flip == 0 else steps:

                def arrive(step=step, flip=flip):
                    x_arrived(tensor, step, flip).wait_recv()
                    c_copy(tensor, step, flip, True).start()

                pl.when(valid(step))(arrive)

    def finish(tensor):
        for flip in (0, 1):
            for plane in range(4):
                owner = plane * 4 + (y + flip - 2 * y * flip) * 2 + (1 - core)
                for kind in (0, 1):
                    first, parts = (2 - 2 * x, 1) if kind else (x, 2)
                    copy(
                        part(tensor, owner, first, parts), part(tensor, owner, first, parts),
                        c_send.at[tensor, kind, flip, plane],
                        c_recv.at[tensor, kind, flip, plane], x, partner,
                    ).wait_recv()
        pltpu.make_async_copy(
            ins[tensor], part(tensor, me, 0, 3), own_sem.at[tensor]
        ).wait()
        for step in steps:

            def sent(step=step):
                if step <= 0:
                    pl.when(z < 3)(lambda: z_copy(tensor, step, True).wait_send())
                if step >= 0:
                    pl.when(z > 0)(lambda: z_copy(tensor, step, False).wait_send())
                y_copy(tensor, step).wait_send()
                for flip in (0, 1):
                    if step != 0 or flip != 0:
                        x_copy(tensor, step, flip).wait_send()
                    for crossed in (False, True):
                        c_copy(tensor, step, flip, crossed).wait_send()

            pl.when(valid(step))(sent)

    begin(0)
    for tensor in range(count):
        if tensor + 1 < count:
            begin(tensor + 1)
        along_z(tensor)
        across_y(tensor)
        if tensor > 0:
            across_x(tensor - 1)
    across_x(count - 1)
    for tensor in range(count):
        finish(tensor)


def tuned(shape):
    return shape["dp"] == 2 and shape["fsdp"] == 16


def gather(shards, shape, identity):
    if not tuned(shape):
        return [lax.all_gather(shard, "fsdp", axis=0, tiled=True) for shard in shards]
    count = len(shards)
    size = shape["fsdp"]
    dma = pltpu.SemaphoreType.DMA
    return pl.pallas_call(
        functools.partial(gather_kernel, count),
        out_shape=[
            jax.ShapeDtypeStruct((size * shard.shape[0], shard.shape[1]), shard.dtype)
            for shard in shards
        ],
        in_specs=[pl.BlockSpec(memory_space=pltpu.VMEM)] * count,
        out_specs=[pl.BlockSpec(memory_space=pl.ANY)] * count,
        scratch_shapes=[
            dma((count,)),
            dma((count, 4)), dma((count, 4)), dma((count, 4)),
            dma((count, 4)), dma((count, 4)),
            dma((count, 2, 4)), dma((count, 2, 4)),
            dma((count, 2, 2, 4)), dma((count, 2, 2, 4)),
        ],
        compiler_params=pltpu.CompilerParams(
            collective_id=identity, has_side_effects=True, vmem_limit_bytes=VMEM_LIMIT
        ),
        name="gather_weights",
    )(*shards)


def pair_up(shape, bit):
    return [(i, i ^ bit) for i in range(shape["fsdp"])]


def add(a, b):
    return (a.astype(F32) + b.astype(F32)).astype(BF)


def pick(array, index, axis):
    return lax.dynamic_index_in_dim(array, index, axis, keepdims=False)


def reduce_scatter(grads, shape):
    size = shape["fsdp"]
    rows = grads.shape[0] // size
    width = grads.shape[1]
    if not tuned(shape):
        part = lax.psum_scatter(grads.astype(F32), "fsdp", scatter_dimension=0, tiled=True)
        return lax.psum(part, "dp")
    third = rows // 3
    x = lax.axis_index("dp")
    me = lax.axis_index("fsdp")
    z, y, core = me // 4, (me // 2) % 2, me % 2
    swap = [(0, 1), (1, 0)]
    grid = grads.reshape(4, 2, 2, rows, width)
    part = add(
        pick(grid, core, 2), lax.ppermute(pick(grid, 1 - core, 2), "fsdp", pair_up(shape, 1))
    )
    crossed = lax.ppermute(
        lax.dynamic_slice_in_dim(part, (1 - x) * 2 * third, third, 2), "dp", swap
    ).astype(F32)
    kept = lax.dynamic_slice_in_dim(part, x * third, 2 * third, 2).astype(F32)
    kept = jnp.concatenate(
        [
            kept[:, :, :third] + jnp.where(x == 0, crossed, 0.0),
            kept[:, :, third:] + jnp.where(x == 1, crossed, 0.0),
        ],
        2,
    ).astype(BF)
    kept = add(pick(kept, y, 1), lax.ppermute(pick(kept, 1 - y, 1), "fsdp", pair_up(shape, 2)))
    kept = kept.reshape(2, 2, 2 * third, width)
    low, high = z % 2, z // 2
    kept = add(pick(kept, low, 1), lax.ppermute(pick(kept, 1 - low, 1), "fsdp", pair_up(shape, 4)))
    kept = add(
        pick(kept, high, 0), lax.ppermute(pick(kept, 1 - high, 0), "fsdp", pair_up(shape, 8))
    )
    other = lax.ppermute(kept, "dp", swap).astype(F32)
    kept = kept.astype(F32)
    front = x == 0
    return jnp.concatenate(
        [
            jnp.where(front, kept[:third], other[:third]),
            jnp.where(front, kept[third:] + other[:third], kept[:third] + other[third:]),
            jnp.where(front, other[third:], kept[third:]),
        ],
        0,
    )


def collect(rows, shape):
    rows = rows[None]
    if not tuned(shape):
        return lax.all_gather(rows, ("dp", "fsdp"), axis=0, tiled=True)
    rows = jnp.concatenate([rows, lax.ppermute(rows, "dp", [(0, 1), (1, 0)])], 0)
    for bit in (2, 4, 8, 1):
        rows = jnp.concatenate([rows, lax.ppermute(rows, "fsdp", pair_up(shape, bit))], 0)
    return rows


def swap_halves(values):
    width = values.shape[1]
    ahead = pltpu.roll(values, width - HD // 2, 1)
    behind = pltpu.roll(values, HD // 2, 1)
    low = lax.broadcasted_iota(jnp.int32, values.shape, 1) % HD < HD // 2
    return jnp.where(low, ahead, behind)


def project_kernel(x_ref, mask_ref, rows_ref, weight_ref, cos_ref, sin_ref, n_ref, q_ref, k_ref, v_ref):
    values = jnp.where(mask_ref[...] == 1, rows_ref[2:3], x_ref[...].astype(F32))
    mean = jnp.mean(values, -1, keepdims=True)
    centered = values - mean
    variance = jnp.mean(centered * centered, -1, keepdims=True)
    normed = (centered * lax.rsqrt(variance + 1e-05) * rows_ref[0:1] + rows_ref[1:2]).astype(BF)
    n_ref[...] = normed
    cosine, sine = cos_ref[...], sin_ref[...]
    for index, out in enumerate((q_ref, k_ref)):
        united = dot(normed, weight_ref[:, index * D : (index + 1) * D])
        factor = HD**-0.5 * LOG2E if index == 0 else None
        for start in range(0, D, PAIR):
            cut = united[:, start : start + PAIR]
            turned = cut * cosine + swap_halves(cut) * sine
            if factor is not None:
                turned = turned * factor
            out[:, start : start + PAIR] = turned.astype(BF)
    v_ref[...] = dot(normed, weight_ref[:, 2 * D :]).astype(BF)


def project(x, mask, rows, weight, cosine, sine, block=256):
    length = x.shape[0]
    wide = pl.BlockSpec((block, D), lambda i: (i, 0))
    table = pl.BlockSpec((block, PAIR), lambda i: (i, 0))
    return pl.pallas_call(
        project_kernel,
        grid=(length // block,),
        in_specs=[
            wide,
            pl.BlockSpec((block, 1), lambda i: (i, 0)),
            pl.BlockSpec((8, D), lambda i: (0, 0)),
            pl.BlockSpec((D, 3 * D), lambda i: (0, 0)),
            table,
            table,
        ],
        out_specs=[wide] * 4,
        out_shape=[jax.ShapeDtypeStruct((length, D), BF)] * 4,
        compiler_params=pltpu.CompilerParams(vmem_limit_bytes=VMEM_LIMIT),
        cost_estimate=pl.CostEstimate(
            flops=2 * length * D * 3 * D, bytes_accessed=14 << 20, transcendentals=0
        ),
        name="project",
    )(x, mask, rows, weight, cosine, sine)


def low_head(shape):
    return lax.broadcasted_iota(jnp.int32, shape, 1) % PAIR < HD


def attend_kernel(q_ref, k_ref, v_ref, o_ref, r_ref, e_ref):
    keys, values, queries = k_ref[...], v_ref[...], q_ref[...]
    length = keys.shape[0]
    low = low_head(keys.shape)
    zero = jnp.zeros_like(keys)
    split_keys = (jnp.where(low, keys, zero), jnp.where(low, zero, keys))
    turned = values.T
    ones = jnp.ones((16, length), BF)
    outs, inverses = [], []
    for head in range(2):
        scores = dot_nt(split_keys[head], queries)
        top = jnp.max(scores, 0, keepdims=True)
        expo = jnp.exp2(scores - top).astype(BF)
        e_ref[head] = expo
        mixed = dot(
            jnp.concatenate([turned[HD * head : HD * (head + 1)], ones], 0), expo
        )
        inverse = 1.0 / mixed[HD : HD + 1]
        outs.append(mixed[:HD] * inverse)
        inverses.append(jnp.broadcast_to(inverse, (HD, length)))
    o_ref[...] = jnp.concatenate(outs, 0).T.astype(BF)
    r_ref[...] = jnp.concatenate(inverses, 0).T


def attend(queries, keys, values):
    length = queries.shape[0]
    pairs = D // PAIR
    cut = pl.BlockSpec((length, PAIR), lambda p: (0, p))
    return pl.pallas_call(
        attend_kernel,
        grid=(pairs,),
        in_specs=[cut] * 3,
        out_specs=[cut, cut, pl.BlockSpec((2, length, length), lambda p: (p, 0, 0))],
        out_shape=[
            jax.ShapeDtypeStruct((length, D), BF),
            jax.ShapeDtypeStruct((length, D), F32),
            jax.ShapeDtypeStruct((2 * pairs, length, length), BF),
        ],
        compiler_params=pltpu.CompilerParams(vmem_limit_bytes=VMEM_LIMIT),
        cost_estimate=pl.CostEstimate(
            flops=16 * length * length * D, bytes_accessed=34 << 20, transcendentals=0
        ),
        name="attend",
    )(queries, keys, values)


def attend_back_kernel(
    block, q_ref, k_ref, v_ref, g_ref, o_ref, r_ref, e_ref, cos_ref, sin_ref,
    dq_ref, dk_ref, dv_ref, dk_sum, dv_sum,
):
    keys, values = k_ref[...], v_ref[...]
    length = keys.shape[0]
    low = low_head(keys.shape)
    zero = jnp.zeros_like(keys)
    split_values = (jnp.where(low, values, zero), jnp.where(low, zero, values))
    turned = keys.T
    low = low_head((block, PAIR))
    for step in range(length // block):
        rows = slice(step * block, (step + 1) * block)
        queries = q_ref[rows, :]
        scaled = g_ref[rows, :].astype(F32) * r_ref[rows, :]
        upstream = scaled.astype(BF)
        products = (scaled * o_ref[rows, :].astype(F32)).T
        zero = jnp.zeros_like(upstream)
        split_up = (jnp.where(low, upstream, zero), jnp.where(low, zero, upstream))
        split_queries = (jnp.where(low, queries, zero), jnp.where(low, zero, queries))
        turned_grads = []
        value_part = key_part = None
        for head in range(2):
            cut = slice(HD * head, HD * (head + 1))
            delta = jnp.sum(products[cut], 0, keepdims=True)
            expo = e_ref[head, :, rows]
            dprobs = dot_nt(split_values[head], upstream)
            score_grad = (expo.astype(F32) * (dprobs - delta)).astype(BF)
            value_term = dot(expo, split_up[head])
            key_term = dot(score_grad, split_queries[head])
            value_part = value_term if head == 0 else value_part + value_term
            key_part = key_term if head == 0 else key_part + key_term
            turned_grads.append(dot(turned[cut], score_grad))
        if step == 0:
            dv_sum[...] = value_part
            dk_sum[...] = key_part
        else:
            dv_sum[...] += value_part
            dk_sum[...] += key_part
        grads = jnp.concatenate(turned_grads, 0).T * HD**-0.5
        dq_ref[rows, :] = (
            grads * cos_ref[rows, :] - swap_halves(grads) * sin_ref[rows, :]
        ).astype(BF)
    grads = dk_sum[...] * LN2
    dk_ref[...] = (grads * cos_ref[...] - swap_halves(grads) * sin_ref[...]).astype(BF)
    dv_ref[...] = dv_sum[...].astype(BF)


def attend_back(queries, keys, values, upstream, attended, inverse, expo, cosine, sine, block=512):
    length = queries.shape[0]
    pairs = D // PAIR
    cut = pl.BlockSpec((length, PAIR), lambda p: (0, p))
    table = pl.BlockSpec((length, PAIR), lambda p: (0, 0))
    return pl.pallas_call(
        functools.partial(attend_back_kernel, block),
        grid=(pairs,),
        in_specs=[cut] * 6
        + [pl.BlockSpec((2, length, length), lambda p: (p, 0, 0)), table, table],
        out_specs=[cut] * 3,
        out_shape=[jax.ShapeDtypeStruct((length, D), BF)] * 3,
        scratch_shapes=[pltpu.VMEM((length, PAIR), F32)] * 2,
        compiler_params=pltpu.CompilerParams(vmem_limit_bytes=VMEM_LIMIT),
        cost_estimate=pl.CostEstimate(
            flops=24 * length * length * D, bytes_accessed=40 << 20, transcendentals=0
        ),
        name="attend_back",
    )(queries, keys, values, upstream, attended, inverse, expo, cosine, sine)


def expand_kernel(n_ref, weight_ref, bias_ref, a_ref, s_ref):
    u = dot(n_ref[...], weight_ref[...]) + bias_ref[...]
    c = math.sqrt(2.0 / math.pi)
    square = u * u
    half = 0.5 + 0.5 * jnp.tanh(u * (c + (c * 0.044715) * square))
    active = u * half
    a_ref[...] = active.astype(BF)
    slope = half + active * (1.0 - half) * (2.0 * c + (6.0 * c * 0.044715) * square)
    s_ref[...] = slope.astype(BF)


def expand(normed, weight, bias, block=512):
    length = normed.shape[0]
    hidden = weight.shape[1]
    out = pl.BlockSpec((length, block), lambda i: (0, i))
    return pl.pallas_call(
        expand_kernel,
        grid=(hidden // block,),
        in_specs=[
            pl.BlockSpec((length, D), lambda i: (0, 0)),
            pl.BlockSpec((D, block), lambda i: (0, i)),
            pl.BlockSpec((1, block), lambda i: (0, i)),
        ],
        out_specs=[out, out],
        out_shape=[jax.ShapeDtypeStruct((length, hidden), BF)] * 2,
        compiler_params=pltpu.CompilerParams(vmem_limit_bytes=VMEM_LIMIT),
        cost_estimate=pl.CostEstimate(
            flops=2 * length * D * hidden, bytes_accessed=19 << 20, transcendentals=0
        ),
        name="expand",
    )(normed, weight, bias)


def expand_back_kernel(g_ref, weight_ref, s_ref, e_ref, t_ref):
    grads = (dot_nt(g_ref[...], weight_ref[...]) * s_ref[...].astype(F32)).astype(BF)
    e_ref[...] = grads
    t_ref[...] = jnp.sum(grads.astype(F32), 0, keepdims=True)


def expand_back(branch_grad, weight, slope, block=512):
    length, hidden = slope.shape
    wide = pl.BlockSpec((length, block), lambda i: (0, i))
    return pl.pallas_call(
        expand_back_kernel,
        grid=(hidden // block,),
        in_specs=[
            pl.BlockSpec((length, D), lambda i: (0, 0)),
            pl.BlockSpec((block, D), lambda i: (i, 0)),
            wide,
        ],
        out_specs=[wide, pl.BlockSpec((1, block), lambda i: (0, i))],
        out_shape=[
            jax.ShapeDtypeStruct((length, hidden), BF),
            jax.ShapeDtypeStruct((1, hidden), F32),
        ],
        compiler_params=pltpu.CompilerParams(vmem_limit_bytes=VMEM_LIMIT),
        cost_estimate=pl.CostEstimate(
            flops=2 * length * D * hidden, bytes_accessed=19 << 20, transcendentals=0
        ),
        name="expand_back",
    )(branch_grad, weight, slope)


def normalise(values):
    mean = jnp.mean(values, -1, keepdims=True)
    centered = values - mean
    variance = jnp.mean(centered * centered, -1, keepdims=True)
    inverse = lax.rsqrt(variance + 1e-05)
    return centered * inverse, inverse


def norm_back(grads, normal, inverse, gain, scale):
    shift_grad = jnp.sum(grads, 0)
    product = jnp.sum(grads * normal, 0)
    scale_grad = product * gain
    gain_grad = product * (1.0 + scale)
    dz = grads * ((1.0 + scale) * gain)
    input_grad = inverse * (
        dz - jnp.mean(dz, -1, keepdims=True) - normal * jnp.mean(dz * normal, -1, keepdims=True)
    )
    return input_grad, shift_grad, scale_grad, gain_grad


def shards(
    shape, hidden_states, condition, absorbed, positions, modulator, offsets, prescale, projector,
    merger, midscale, expander, thresholds, contractor, baseline, absorber, cotangent,
):
    size = shape["fsdp"]
    me = lax.axis_index("fsdp")
    x = hidden_states[0]
    length = x.shape[0]
    vectors = (offsets, prescale, midscale, thresholds, baseline, absorber)
    packed = jnp.concatenate(vectors)
    rows = 6 * modulator.shape[0]
    packed = jnp.pad(packed, (0, rows * 128 - packed.shape[0])).reshape(rows, 128)
    packed = jnp.concatenate([modulator.reshape(rows, D), packed], 1)
    full_pack, full_projector, full_merger, full_expander, full_contractor = gather(
        (packed, projector, merger, expander, contractor), shape, 1
    )
    full_modulator = full_pack[:, :D]
    tail = full_pack[:, D:].reshape(size, rows * 128)
    full, start = [], 0
    for vector in vectors:
        width = vector.shape[0]
        full.append(tail[:, start : start + width].reshape(-1).astype(F32))
        start += width
    full_offsets, full_prescale, full_midscale, full_thresholds, full_baseline, full_absorber = full

    cond_float = condition[0].astype(F32)
    silu_cond = jax.nn.silu(cond_float).astype(BF)
    six = lax.broadcasted_iota(jnp.int32, (6, full_modulator.shape[0]), 1) % 6
    chosen = six == lax.broadcasted_iota(jnp.int32, six.shape, 0)
    spread = jnp.where(chosen, jnp.repeat(silu_cond, 6)[None], jnp.zeros((), BF))
    modulation = dot(spread, full_modulator) + full_offsets.reshape(6, D)
    shift_one, scale_one, gate_one, shift_two, scale_two, gate_two = modulation

    lane = jnp.arange(PAIR)
    inverse_rate = 10000.0 ** (-(lane % (HD // 2)).astype(F32) / (HD // 2))
    angles = positions[0].astype(F32)[:, None] * inverse_rate
    cosine = jnp.cos(angles)
    sine = jnp.where(lane % HD < HD // 2, -1.0, 1.0) * jnp.sin(angles)

    mask = absorbed[0][:, None]
    first_rows = jnp.concatenate(
        [
            (full_prescale * (1.0 + scale_one))[None],
            shift_one[None],
            full_absorber[None],
            jnp.zeros((5, D), F32),
        ],
        0,
    )
    normed_one, queries, keys, values = project(
        x, mask, first_rows, full_projector, cosine, sine
    )
    attended, inverse, expo = attend(queries, keys, values)
    branch_one = dot(attended, full_merger)
    block_in = jnp.where(mask == 1, full_absorber, x.astype(F32))
    middle = block_in + gate_one * branch_one
    normal_two, spread_two = normalise(middle)
    normed_two = (normal_two * (full_midscale * (1.0 + scale_two)) + shift_two).astype(BF)
    activated, slope = expand(normed_two, full_expander, full_thresholds[None])
    branch_two = dot(activated, full_contractor) + full_baseline
    block_output = (middle + gate_two * branch_two).astype(BF)

    upstream = cotangent[0].astype(F32)
    grad_gate_two = jnp.sum(upstream * branch_two, 0)
    branch_grad = (upstream * gate_two).astype(BF)
    grad_baseline = jnp.sum(branch_grad.astype(F32), 0)
    grad_contractor = reduce_scatter(dot_tn(activated, branch_grad).astype(BF), shape)
    expand_grad, grad_thresholds = expand_back(branch_grad, full_contractor, slope)
    grad_expander = reduce_scatter(dot_tn(normed_two, expand_grad).astype(BF), shape)
    normed_two_grad = dot_nt(expand_grad, full_expander)
    middle_grad, grad_shift_two, grad_scale_two, grad_midscale = norm_back(
        normed_two_grad, normal_two, spread_two, full_midscale, scale_two
    )
    middle_grad = middle_grad + upstream
    grad_gate_one = jnp.sum(middle_grad * branch_one, 0)
    merged_grad = (middle_grad * gate_one).astype(BF)
    grad_merger = reduce_scatter(dot_tn(attended, merged_grad).astype(BF), shape)
    attended_grad = dot_nt(merged_grad, full_merger).astype(BF)
    early = collect(
        jnp.concatenate(
            [
                grad_gate_one, grad_shift_two, grad_scale_two, grad_gate_two, grad_thresholds[0],
                grad_midscale, grad_baseline, silu_cond.astype(F32),
            ]
        ).astype(BF),
        shape,
    )
    united_grads = attend_back(
        queries, keys, values, attended_grad, attended, inverse, expo, cosine, sine
    )
    grad_projector = jnp.concatenate(
        [
            reduce_scatter(dot_tn(normed_one, grads).astype(BF), shape) for grads in united_grads
        ],
        1,
    )
    normed_one_grad = sum(
        dot_nt(grads, full_projector[:, i * D : (i + 1) * D])
        for i, grads in enumerate(united_grads)
    )
    normal_one, spread_one = normalise(block_in)
    input_grad, grad_shift_one, grad_scale_one, grad_prescale = norm_back(
        normed_one_grad, normal_one, spread_one, full_prescale, scale_one
    )
    input_grad = input_grad + middle_grad
    grad_hidden = jnp.where(mask == 1, 0.0, input_grad)
    grad_absorber = jnp.sum(jnp.where(mask == 1, input_grad, 0.0), 0)
    late = collect(
        jnp.concatenate([grad_shift_one, grad_scale_one, grad_prescale, grad_absorber]).astype(BF),
        shape,
    )
    own_modulation = jnp.stack(
        [
            grad_shift_one, grad_scale_one, grad_gate_one, grad_shift_two, grad_scale_two,
            grad_gate_two,
        ]
    )
    spread_grad = lax.dot_general(
        own_modulation, full_modulator.astype(F32), NT, precision=lax.Precision.HIGHEST
    )
    silu_grad = jnp.sum(jnp.where(chosen, spread_grad, 0.0), 0).reshape(-1, 6).sum(1)
    unused_value, silu_back = jax.vjp(jax.nn.silu, cond_float)
    grad_condition = silu_back(silu_grad)[0][None]

    modulations = jnp.concatenate([late[:, : 2 * D], early[:, : 4 * D]], 1)
    hidden = full_thresholds.shape[0]
    width = modulator.shape[0]
    conditions = early[:, 6 * D + hidden :]
    own_conditions = lax.dynamic_slice_in_dim(conditions, me * width, width, 1)
    grad_modulator = dot_tn(own_conditions, modulations)

    def own_sum(rows):
        total = jnp.sum(rows.astype(F32), 0)
        part = total.shape[0] // size
        return lax.dynamic_slice_in_dim(total, me * part, part, 0)

    grad_offsets = own_sum(modulations)
    grad_prescale = own_sum(late[:, 2 * D : 3 * D])
    grad_absorber = own_sum(late[:, 3 * D :])
    grad_thresholds = own_sum(early[:, 4 * D : 4 * D + hidden])
    grad_midscale = own_sum(early[:, 4 * D + hidden : 5 * D + hidden])
    grad_baseline = own_sum(early[:, 5 * D + hidden : 6 * D + hidden])
    return (
        block_output[None], grad_hidden[None], grad_condition, grad_modulator, grad_offsets,
        grad_prescale, grad_projector, grad_merger, grad_midscale, grad_expander,
        grad_thresholds, grad_contractor, grad_baseline, grad_absorber,
    )


def solution(mesh):
    batch, rows, flat = P(("dp", "fsdp")), P("fsdp", None), P("fsdp")
    return jax.shard_map(
        functools.partial(shards, dict(mesh.shape)),
        mesh=mesh,
        in_specs=(
            batch, batch, batch, batch, rows, flat, flat, rows, rows, flat, rows, flat, rows,
            flat, flat, batch,
        ),
        out_specs=(
            batch, batch, batch, rows, flat, flat, rows, rows, flat, rows, flat, rows, flat, flat,
        ),
        check_vma=False,
    )
```
